32 devices in a mesh: shard: 4 (over z), context: 2 (over core), tensor: 4 (over y, x).
Axes of the slice: x: 2, y: 2, z: 4, core: 2. Of those that a mesh axis runs over, the one named last changes fastest.
Arguments:
- tokens: bfloat16 [4, 1024, 2048], P('shard', 'context'), may hold values from -6 to 6
- qkv_weight: bfloat16 [3, 2048, 2048], P(None, 'shard', 'tensor'), may hold values from -0.125 to 0.125
- out_weight: bfloat16 [2048, 2048], P('tensor', 'shard'), may hold values from -0.75 to 0.75
- router_weight: bfloat16 [16, 2048], P(None, 'shard'), may hold values from -0.125 to 0.125
- norm_gains: float32 [2, 2048], replicated, may hold values from 0.5 to 1.5
- qk_gains: float32 [2, 128, 16], P(None, None, 'tensor'), may hold values from 0.5 to 1.5
- gate_up_weight: bfloat16 [16, 2048, 2, 1024], P(None, 'shard', None, 'tensor'), may hold values from -0.125 to 0.125
- down_weight: bfloat16 [16, 2048, 1024], P(None, 'shard', 'tensor'), may hold values from -0.75 to 0.75
- routes: int32 [4, 1024, 8], P('shard', 'context'), may hold values from 0 to 15, all different within a row; in each aligned block of 512 rows (0 to 511, 512 to 1023, ..., all dimensions but the last counted through in order) at most 384 rows name the same one
- segments: int32 [4, 1024], P('shard'), may hold values from 0 to 3, never falling along the last dimension, each value on 1 to 512 neighbouring positions
- cotangent: bfloat16 [4, 1024, 2048], P('shard', 'context'), may hold values from -6 to 6
Outputs:
- output: bfloat16 [4, 1024, 2048], P('shard', 'context')
- input_grad: bfloat16 [4, 1024, 2048], P('shard', 'context')
- qkv_grad: float32 [3, 2048, 2048], P(None, ('shard', 'context'), 'tensor')
- out_grad: float32 [2048, 2048], P('tensor', ('shard', 'context'))
- router_grad: float32 [16, 2048], P(None, ('shard', 'context'))
- gains_grad: float32 [2, 2048], P(None, ('shard', 'context'))
- qk_gains_grad: float32 [2, 128, 16], P(None, ('shard', 'context'), 'tensor')
- gate_up_grad: float32 [16, 2048, 2, 1024], P(None, ('shard', 'context'), None, 'tensor')
- down_grad: float32 [16, 2048, 1024], P(None, ('shard', 'context'), 'tensor')
The draws below stay inside these ranges and needn't reach their ends.
Inputs may be any that keep to these rules, and one draw needn't show every extreme that they name: `routes`: each token names 8 different experts; in each aligned block of 512 tokens no expert is named by more than 384 tokens, and in some blocks one expert is named by exactly 384. `segments`: document ids never fall along a sequence; a document holds at most half of 1024 tokens, and some document holds exactly that many.
All inputs are finite; a program needn't handle non-finite values.
Results may differ from the reference program's by a relative error of at most 0.017.
Values may be sent and summed in bfloat16 or wider, within the bound.
A program may use at most 192 MiB of HBM per device.

```python
import math
import jax
import jax.numpy as jnp
import numpy as np
from jax import lax

D = 2048
HEADS = 16
HEAD_DIM = 128
FF = 1024
EXPERTS = 16
TOPK = 8
SEQ_LEN = 1024
SEQS = 4
ROWS = 512
CAP = 384
DOCS = 4
N_CONTEXT = 2


def block_scale(own_key, shape, shards, least, top_value):
    loudness, own = 1.0, jax.random.fold_in(own_key, 6)
    for dim, parts in shards:
        draws = jnp.exp(jax.random.uniform(jax.random.fold_in(own, dim), (parts,), jnp.float32, least / len(shards), top_value / len(shards)))
        loudness = loudness * jnp.repeat(draws, shape[dim] // parts).reshape([-1 if axis == dim else 1 for axis in range(len(shape))])
    return loudness


def split_up(count, total, reach, lean):
    weights = [(1 << 20) // math.isqrt(rank ** lean) + 1 for rank in range(2, count + 1)]
    surplus, counts = total - reach - (count - 1), [1] * (count - 1)
    while surplus > 0:
        candidates = [i for i in range(count - 1) if counts[i] < reach]
        pool, left = sum([weights[i] for i in candidates]), surplus
        for i in candidates:
            addition = min(reach - counts[i], max(1, left * weights[i] // pool), surplus)
            counts[i] = counts[i] + addition
            surplus = surplus - addition
    return np.array([reach] + counts)


def uneven_parts(stream_key, number_of, total, bound, skew):
    if number_of == 2:
        one = jax.random.randint(stream_key, (), max(1, total - bound), min(bound, total - 1) + 1)
        return jnp.stack([one, total - one])
    sizes = jnp.asarray(split_up(number_of, total, bound, skew), jnp.int32)
    pairs = (number_of - 1) // 2
    donor, sink = sizes[1:1 + 2 * pairs:2], sizes[2:2 + 2 * pairs:2]
    room = jnp.minimum(donor - 1, bound - sink)
    passed = jax.random.randint(jax.random.fold_in(stream_key, 1), (pairs,), 0, 1 << 20) % (room + 1)
    sizes = sizes.at[1:1 + 2 * pairs:2].set(donor - passed).at[2:2 + 2 * pairs:2].set(sink + passed)
    return sizes[jax.random.permutation(jax.random.fold_in(stream_key, 2), number_of)]


def deal_out(stream_key, own, number, rows, number_of, top, reach, skew):
    order = jax.random.permutation(stream_key, number_of)
    crowded, ordinary = portions_of(number_of, rows * top, reach, skew, True), portions_of(number_of, rows * top, reach, skew, False)
    places = jnp.arange(number_of)

    def named(tallies, turn):
        used = int((tallies > 0).sum())
        fixed = max(1, used // 4)
        passed = fixed + (places - fixed + turn * (used - fixed)) % max(1, number_of - fixed)
        return jnp.zeros((number_of,), jnp.int32).at[order[jnp.where(places < fixed, places, passed)]].set(jnp.asarray(tallies, jnp.int32))

    tallies = jnp.where(number % 4 == 0, named(crowded, number // 4), named(ordinary, number - number // 4 - 1))
    mixed = jax.random.permutation(jax.random.fold_in(own, 3), number_of)
    source_of, sink = mixed[0:number_of // 2 * 2:2], mixed[1:number_of // 2 * 2:2]
    margin = jnp.minimum(tallies[source_of] - 1, reach - tallies[sink]) // 2
    margin = jnp.where((source_of == order[0]) | (sink == order[0]) | (tallies[sink] == 0), 0, jnp.maximum(margin, 0))
    passed = jax.random.randint(jax.random.fold_in(own, 4), (number_of // 2,), 0, 1 << 20) % (margin + 1)
    tallies = tallies.at[source_of].add(-passed).at[sink].add(passed)
    items = jnp.searchsorted(jnp.cumsum(tallies), jnp.arange(rows * top), side="right").astype(jnp.int32)
    table = items.reshape(top, rows).T
    table = table[jax.random.permutation(jax.random.fold_in(own, 1), rows)]
    turn = jax.random.randint(jax.random.fold_in(own, 2), (rows, 1), 0, top)
    return jnp.take_along_axis(table, (jnp.arange(top)[None, :] + turn) % top, axis=1)


def portions_of(number_of, total, limit, lean, full):
    loads = [(1 << 20) // math.isqrt(rank ** lean) + 1 for rank in range(1, number_of + 1)]
    largest = limit if full else min(limit, max(-(-total // number_of), total * loads[0] // sum(loads)))
    least = 1 if total - largest >= number_of - 1 else 0
    given, spare = [largest] + [least] * (number_of - 1), total - largest - least * (number_of - 1)
    while spare > 0:
        free = [i for i in range(1, number_of) if given[i] < largest] or [i for i in range(1, number_of) if given[i] < limit]
        pool, budget = sum([loads[i] for i in free]), spare
        for i in free:
            addition = min(limit - given[i], max(1, budget * loads[i] // pool), spare)
            given[i] = given[i] + addition
            spare = spare - addition
    return np.array(given)


def normal_values(key, shape, scale, reach, pieces=(), kind=jnp.bfloat16):
    gain = block_scale(key, shape, pieces, -0.22, 0.18) if pieces else 1.0
    drawn = jax.random.normal(key, shape, jnp.float32) * scale * gain
    return jnp.minimum(jnp.maximum(drawn, -reach), reach).astype(kind)


def setup_inputs(seed: int = 0) -> dict:
    key_of = jax.random.split(jax.random.key(seed), 12)
    tokens = normal_values(key_of[0], (SEQS, SEQ_LEN, D), 1.0, 6.0, ((0, 4), (1, 2)))
    qkv_weight = normal_values(key_of[1], (3, D, D), D ** -0.5, 0.125, ((1, 4), (2, 4)))
    out_weight = normal_values(key_of[2], (D, D), (D // 32) ** -0.5, 0.75, ((0, 4), (1, 4)))
    router_weight = normal_values(key_of[3], (EXPERTS, D), D ** -0.5, 0.125, ((1, 4),))
    norm_gains = jnp.clip(1.0 + 0.1 * jax.random.normal(key_of[4], (2, D), jnp.float32), 0.5, 1.5)
    qk_gains = jnp.clip(1.0 + 0.1 * jax.random.normal(key_of[5], (2, HEAD_DIM, HEADS), jnp.float32), 0.5, 1.5)
    gate_up_weight = normal_values(key_of[6], (EXPERTS, D, 2, FF), D ** -0.5, 0.125, ((1, 4), (3, 4)))
    down_weight = normal_values(key_of[7], (EXPERTS, D, FF), (FF // 16) ** -0.5, 0.75, ((1, 4), (2, 4)))
    routes_keys = jax.random.split(jax.random.fold_in(key_of[8], 1), SEQS * SEQ_LEN // ROWS)
    routes_turns = jax.random.permutation(jax.random.fold_in(key_of[8], 3), SEQS * SEQ_LEN // ROWS)
    routes = jax.vmap(lambda own, number: deal_out(jax.random.fold_in(key_of[8], 2), own, number, ROWS, EXPERTS, TOPK, CAP, 2))(routes_keys, routes_turns).reshape((SEQS, SEQ_LEN, TOPK))
    segments = jax.vmap(lambda own: jnp.searchsorted(jnp.cumsum(uneven_parts(own, DOCS, SEQ_LEN, SEQ_LEN // 2, 1)), jnp.arange(SEQ_LEN), side="right"))(jax.random.split(key_of[9], SEQS)).reshape((SEQS, SEQ_LEN)).astype(jnp.int32)
    cotangent = normal_values(key_of[10], (SEQS, SEQ_LEN, D), 1.0, 6.0, ((0, 4), (1, 2)))
    return dict(tokens=tokens, qkv_weight=qkv_weight, out_weight=out_weight, router_weight=router_weight, norm_gains=norm_gains, qk_gains=qk_gains, gate_up_weight=gate_up_weight, down_weight=down_weight, routes=routes, segments=segments, cotangent=cotangent)


norm_epsilon = 1e-05
rope_base = 10000.0
masked_score = -1e+30
highest = lax.Precision.HIGHEST

@jax.custom_vjp
def low(v):
    return lax.optimization_barrier(v.astype(jnp.bfloat16)).astype(jnp.float32)

@jax.custom_vjp
def low_back(v):
    return v

def low_keep(v):
    return (low(v), None)

def low_pass(kept, grad):
    return (grad,)

def back_keep(v):
    return (v, None)

def back_low(kept, grad):
    return (low(grad),)
low.defvjp(low_keep, low_pass)
low_back.defvjp(back_keep, back_low)

def rms_scale(values):
    return lax.rsqrt(lax.optimization_barrier(jnp.mean(values * values, axis=-1, keepdims=True)) + norm_epsilon)

def softmax_rows(scores):
    shifted = scores - lax.optimization_barrier(jnp.max(scores, axis=-1, keepdims=True))
    raised = jnp.exp(shifted)
    return raised / lax.optimization_barrier(jnp.sum(raised, axis=-1, keepdims=True))

def silu_of(values):
    return values * jax.nn.sigmoid(values)

def doc_positions(segment_rows):
    length = segment_rows.shape[-1]
    docs_list = jnp.arange(DOCS, dtype=jnp.int32)
    member = (segment_rows[..., :, None] == docs_list).astype(jnp.int32)
    sizes_of = lax.optimization_barrier(jnp.sum(member, axis=-2))
    starts = jnp.cumsum(sizes_of, axis=-1) - sizes_of
    start_of = lax.optimization_barrier(jnp.sum(member * starts[..., None, :], axis=-1))
    return jnp.arange(length, dtype=jnp.int32) - start_of

def rotary_tables(positions):
    half_dim = HEAD_DIM // 2
    ladder = jnp.arange(half_dim, dtype=jnp.float32)
    inverse = rope_base ** (-2.0 * ladder / HEAD_DIM)
    angles = positions.astype(jnp.float32)[..., None] * inverse
    angles = jnp.concatenate([angles, angles], axis=-1)
    return (jnp.cos(angles), jnp.sin(angles))

def rotate(values, cosine, sine_table):
    half_dim = values.shape[-1] // 2
    lower_half = values[..., :half_dim]
    upper_half = values[..., half_dim:]
    return values * cosine + jnp.concatenate([-upper_half, lower_half], axis=-1) * sine_table

def dispatch(block_routes):
    block_rows, pick_count = block_routes.shape
    expert_ids = jnp.arange(EXPERTS, dtype=jnp.int32)
    flat_routes = block_routes.reshape(-1)
    member = (flat_routes[:, None] == expert_ids[None, :]).astype(jnp.int32)
    before = jnp.cumsum(member, axis=0) - member
    rank_of = lax.optimization_barrier(jnp.sum(before * member, axis=1))
    target = flat_routes * CAP + rank_of
    filler = jnp.full((EXPERTS * CAP,), block_rows * pick_count, jnp.int32)
    slot_table = filler.at[target].set(jnp.arange(block_rows * pick_count, dtype=jnp.int32))
    slot_table = slot_table.reshape(EXPERTS, CAP)
    return (slot_table // pick_count, slot_table)

def expert_tables(route_blocks):
    block_count, block_rows, pick_count = route_blocks.shape
    row_table, pick_table = jax.vmap(dispatch)(route_blocks)
    offsets = jnp.arange(block_count, dtype=jnp.int32)[:, None, None]
    row_table = jnp.where(row_table < block_rows, row_table + offsets * block_rows, block_count * block_rows)
    pick_table = jnp.where(pick_table < block_rows * pick_count, pick_table + offsets * block_rows * pick_count, block_count * block_rows * pick_count)
    row_table = row_table.transpose(1, 0, 2).reshape(EXPERTS, block_count * CAP)
    pick_table = pick_table.transpose(1, 0, 2).reshape(EXPERTS, block_count * CAP)
    return (row_table, pick_table)

def attend_sequence(queries, keys, values, segment_row):
    length = segment_row.shape[0]
    scores = jnp.einsum('qhd,khd->hqk', queries, keys, precision=highest) * HEAD_DIM ** (-0.5)
    scores = low_back(scores)
    places = jnp.arange(length, dtype=jnp.int32)
    allowed = (segment_row[:, None] == segment_row[None, :]) & (places[:, None] >= places[None, :])
    scores = jnp.where(allowed[None], scores, masked_score)
    weights = low(softmax_rows(scores))
    attended = jnp.einsum('hqk,khd->qhd', weights, values, precision=highest)
    return low(low_back(attended))

def forward(tokens, qkv_weight, out_weight, router_weight, norm_gains, qk_gains, gate_up_weight, down_weight, row_table, pick_table, routes, segments):
    token_count = SEQS * SEQ_LEN
    flat_tokens = tokens.reshape(token_count, D)
    inputs = low(flat_tokens * rms_scale(flat_tokens) * norm_gains[0])
    projected = low_back(jnp.einsum('td,cde->cte', inputs, qkv_weight, precision=highest))
    query_gain = qk_gains[0].T.reshape(D)
    key_gain = qk_gains[1].T.reshape(D)
    queries = projected[0] * rms_scale(projected[0]) * query_gain
    keys = projected[1] * rms_scale(projected[1]) * key_gain
    cosine, sine_table = rotary_tables(doc_positions(segments).reshape(token_count))
    cosine = cosine[:, None, :]
    sine_table = sine_table[:, None, :]
    shape_heads = (SEQS, SEQ_LEN, HEADS, HEAD_DIM)
    queries = low(rotate(queries.reshape(token_count, HEADS, HEAD_DIM), cosine, sine_table)).reshape(shape_heads)
    keys = low(rotate(keys.reshape(token_count, HEADS, HEAD_DIM), cosine, sine_table)).reshape(shape_heads)
    values = low(projected[2]).reshape(shape_heads)

    def scan_step(running, sequence):
        return (running, jax.checkpoint(attend_sequence)(*sequence))
    unused, attended = lax.scan(scan_step, jnp.zeros((), jnp.float32), (queries, keys, values, segments))
    attended = attended.reshape(token_count, D)
    attn_out = low_back(jnp.dot(attended, out_weight, precision=highest, preferred_element_type=jnp.float32))
    hidden_state = flat_tokens + attn_out
    normed = low(hidden_state * rms_scale(hidden_state) * norm_gains[1])
    logits = low_back(jnp.einsum('td,ed->te', normed, router_weight, precision=highest))
    router_probs = softmax_rows(logits)
    chosen = jnp.take_along_axis(router_probs, routes.reshape(token_count, TOPK), axis=1)
    normed_pad = jnp.concatenate([normed, jnp.zeros((1, D), normed.dtype)], axis=0)
    chosen_pad = jnp.concatenate([chosen.reshape(-1), jnp.zeros((1,), chosen.dtype)])

    def expert_step(mixed_sum, expert_item):
        gate_up, down_piece, row_ids, pick_ids = expert_item
        picked = normed_pad[row_ids]
        gate_up_out = low_back(jnp.einsum('cd,dgf->cgf', picked, gate_up, precision=highest))
        hidden_units = low(silu_of(gate_up_out[:, 0]) * gate_up_out[:, 1])
        expert_out = low_back(jnp.einsum('cf,df->cd', hidden_units, down_piece, precision=highest))
        return (mixed_sum.at[row_ids].add(chosen_pad[pick_ids][:, None] * expert_out), None)
    mixed_sum, unused_too = lax.scan(jax.checkpoint(expert_step), jnp.zeros((token_count + 1, D), jnp.float32), (gate_up_weight, down_weight, row_table, pick_table))
    return (hidden_state + mixed_sum[:token_count]).reshape(SEQS, SEQ_LEN, D)

def reference(tokens, qkv_weight, out_weight, router_weight, norm_gains, qk_gains, gate_up_weight, down_weight, routes, segments, cotangent):
    route_blocks = routes.reshape(SEQS * N_CONTEXT, SEQ_LEN // N_CONTEXT, TOPK)
    row_table, pick_table = expert_tables(route_blocks)
    floats = [operand.astype(jnp.float32) for operand in (tokens, qkv_weight, out_weight, router_weight, norm_gains, qk_gains, gate_up_weight, down_weight)]

    def closed(*weights):
        return forward(*weights, row_table, pick_table, routes, segments)
    output, pullback = jax.vjp(closed, *floats)
    gradients = pullback(cotangent.astype(jnp.float32))
    return (output.astype(jnp.bfloat16), gradients[0].astype(jnp.bfloat16), gradients[1], gradients[2], gradients[3], gradients[4], gradients[5], gradients[6], gradients[7])
```

```python
import jax
import jax.numpy as jnp
from jax import lax
from jax.sharding import PartitionSpec as P

HEAD_DIM = 128
EXPERTS = 16
DOCS = 4


norm_epsilon = 1e-05
rope_base = 10000.0
masked_score = -1e30


def rms_scale(values):
    return lax.rsqrt(jnp.mean(values * values, axis=-1, keepdims=True) + norm_epsilon)


def softmax_rows(scores):
    shifted = scores - jnp.max(scores, axis=-1, keepdims=True)
    raised = jnp.exp(shifted)
    return raised / jnp.sum(raised, axis=-1, keepdims=True)


def silu_of(values):
    return values * jax.nn.sigmoid(values)


def doc_positions(segment_rows):
    length = segment_rows.shape[-1]
    docs_list = jnp.arange(DOCS, dtype=jnp.int32)
    member = (segment_rows[..., :, None] == docs_list).astype(jnp.int32)
    sizes_of = jnp.sum(member, axis=-2)
    starts = jnp.cumsum(sizes_of, axis=-1) - sizes_of
    start_of = jnp.sum(member * starts[..., None, :], axis=-1)
    return jnp.arange(length, dtype=jnp.int32) - start_of


def rotary_tables(positions):
    half_dim = HEAD_DIM // 2
    ladder = jnp.arange(half_dim, dtype=jnp.float32)
    inverse = rope_base ** (-2.0 * ladder / HEAD_DIM)
    angles = positions.astype(jnp.float32)[..., None] * inverse
    angles = jnp.concatenate([angles, angles], axis=-1)
    return (jnp.cos(angles), jnp.sin(angles))


def rotate(values, cosine, sine_table):
    half_dim = values.shape[-1] // 2
    lower_half = values[..., :half_dim]
    upper_half = values[..., half_dim:]
    return values * cosine + jnp.concatenate([-upper_half, lower_half], axis=-1) * sine_table


def rotate_back(grad_values, cosine, sine_table):
    half_dim = grad_values.shape[-1] // 2
    turned = grad_values * sine_table
    return grad_values * cosine + jnp.concatenate(
        [turned[..., half_dim:], -turned[..., :half_dim]], axis=-1
    )


def norm_back(grad_hat, normed_hat, row_scale):
    return row_scale * (
        grad_hat - normed_hat * jnp.mean(grad_hat * normed_hat, axis=-1, keepdims=True)
    )


def passed_along(value, axis, by):
    length = lax.axis_size(axis)
    pairs = [(i, i + by) for i in range(length) if 0 <= i + by < length]
    return lax.ppermute(value, axis, pairs)


def crossed(value, axis, mask):
    length = lax.axis_size(axis)
    return lax.ppermute(value, axis, [(i, i ^ mask) for i in range(length)])


def block_at(value, index, size, axis):
    return lax.dynamic_slice_in_dim(value, index * size, size, axis=axis)


def put_at(whole, part, start, axis):
    return lax.dynamic_update_slice_in_dim(whole, part, start, axis=axis)


def assemble(piece, axis, shard_index, context_index, targets=None):
    shards = lax.axis_size("shard")
    size = (piece if targets is None else targets(0)).shape[axis]
    half = size // 2
    shape = list((piece if targets is None else targets(0)).shape)
    shape[axis] = size * shards
    whole = jnp.zeros(shape, piece.dtype)
    own = piece if targets is None else targets(shard_index)
    whole = put_at(whole, own, shard_index * size, axis)
    for mask in range(1, shards):
        partner = shard_index ^ mask
        block = piece if targets is None else targets(partner)
        came = crossed(block_at(block, context_index, half, axis), "shard", mask)
        other = crossed(came, "context", 1)
        whole = put_at(whole, came, partner * size + context_index * half, axis)
        whole = put_at(whole, other, partner * size + (1 - context_index) * half, axis)
    return whole


def spread_ranks(part, rank):
    rows, width = part.shape
    ranks = lax.axis_size("tensor")
    whole = jnp.zeros((rows, ranks * width), part.dtype)
    whole = put_at(whole, part, rank * width, 1)
    for mask in range(1, ranks):
        whole = put_at(whole, crossed(part, "tensor", mask), (rank ^ mask) * width, 1)
    return whole


def sum_ranks(value, rank):
    ranks = lax.axis_size("tensor")
    width = value.shape[1] // ranks
    total = block_at(value, rank, width, 1).astype(jnp.float32)
    for mask in range(1, ranks):
        came = crossed(block_at(value, rank ^ mask, width, 1), "tensor", mask)
        total = total + came.astype(jnp.float32)
    return total


def total_over(value, axis):
    total = value
    for mask in range(1, lax.axis_size(axis)):
        total = total + crossed(value, axis, mask)
    return total


def tree_total(value, axis):
    mask = 1
    while mask < lax.axis_size(axis):
        value = value + crossed(value, axis, mask)
        mask = mask * 2
    return value


def column_half(value, part, shards):
    size = value.shape[1] // (2 * shards)
    return jnp.concatenate(
        [lax.dynamic_slice_in_dim(value, (2 * p + part) * size, size, axis=1) for p in range(shards)],
        axis=1,
    )


def half_product(left, right, part):
    return lax.dot_general(
        column_half(left, part, lax.axis_size("shard")),
        right,
        (((0,), (0,)), ((), ())),
        preferred_element_type=jnp.float32,
    )


def joined_halves(give, keep):
    return keep + crossed(give.astype(jnp.bfloat16), "context", 1).astype(jnp.float32)


def shared_gradient(left, right, shard_index, context_index):
    give = half_product(left, right, 1 - context_index)
    keep = half_product(left, right, context_index)
    return joined_halves(give, keep)


def shard_sum(value, axis, shard_index):
    shards = lax.axis_size("shard")
    size = value.shape[axis] // shards
    low = value.astype(jnp.bfloat16)
    total = block_at(value, shard_index, size, axis)
    for mask in range(1, shards):
        came = crossed(block_at(low, shard_index ^ mask, size, axis), "shard", mask)
        total = total + came.astype(jnp.float32)
    return total


def expert_shares(value, shard_index, own_experts):
    shards = lax.axis_size("shard")
    rows = value.shape[0] // shards
    width = value.shape[1]
    low = value.astype(jnp.bfloat16)
    result = jnp.zeros((shards, rows, width), jnp.float32)
    result = put_at(result, block_at(value, shard_index, rows, 0)[None], shard_index, 0)
    for mask in range(1, shards):
        partner = shard_index ^ mask
        came = crossed(block_at(low, partner, rows, 0), "shard", mask)
        result = put_at(result, came.astype(jnp.float32)[None], partner, 0)
    return result


def local(
    tokens,
    qkv_weight,
    out_weight,
    router_weight,
    norm_gains,
    qk_gains,
    gate_up_weight,
    down_weight,
    routes,
    segments,
    cotangent,
):
    seq_count, row_count, model_width = tokens.shape
    token_count = seq_count * row_count
    top_count = routes.shape[2]
    local_width = qkv_weight.shape[2]
    head_count = local_width // HEAD_DIM
    shards = lax.axis_size("shard")
    ranks = lax.axis_size("tensor")
    own_experts = EXPERTS // shards
    unit_count = down_weight.shape[2]
    wide = own_experts * unit_count
    slice_width = model_width // ranks
    context_index = lax.axis_index("context")
    shard_index = lax.axis_index("shard")
    rank = lax.axis_index("tensor")

    def my_slice(value, axis):
        return block_at(value, rank, slice_width, axis)

    qkv_full = assemble(qkv_weight, 1, shard_index, context_index)
    out_full = assemble(out_weight, 1, shard_index, context_index)
    router_size = router_weight.shape[1]
    router_full = jnp.zeros((EXPERTS, model_width), router_weight.dtype)
    router_full = put_at(router_full, router_weight, shard_index * router_size, 1)
    for mask in range(1, shards):
        came = crossed(router_weight, "shard", mask)
        router_full = put_at(router_full, came, (shard_index ^ mask) * router_size, 1)
    route_rows = routes.reshape(token_count, top_count)
    grad_low = cotangent.reshape(token_count, model_width)
    grad_slice = my_slice(grad_low, 1)
    streamed = shards * token_count * model_width > 8 * 1024 * 1024
    grad_chunks = [grad_low]
    if not streamed:
        grad_chunks = grad_chunks + [
            spread_ranks(crossed(grad_slice, "shard", mask), rank) for mask in range(1, shards)
        ]
    route_chunks = [route_rows] + [crossed(route_rows, "shard", mask) for mask in range(1, shards)]
    up_lines = gate_up_weight.transpose(1, 2, 0, 3).reshape(-1, 2, shards, wide)
    down_lines = down_weight.transpose(1, 0, 2).reshape(-1, shards, wide)

    def up_block(target):
        return lax.dynamic_index_in_dim(up_lines, target, 2, False).reshape(-1, 2 * wide)

    def down_block(target):
        return lax.dynamic_index_in_dim(down_lines, target, 1, False)

    up_full = assemble(up_lines, 0, shard_index, context_index, up_block)
    down_full = assemble(down_lines, 0, shard_index, context_index, down_block)

    flat_tokens = tokens.reshape(token_count, model_width).astype(jnp.float32)
    scale_one = rms_scale(flat_tokens)
    hat_one = flat_tokens * scale_one
    inputs = (hat_one * norm_gains[0]).astype(jnp.bfloat16)
    projected = jnp.einsum("td,cde->cte", inputs, qkv_full, preferred_element_type=jnp.float32)
    square_sums = total_over(jnp.sum(projected[:2] * projected[:2], axis=-1), "tensor")
    query_scale = lax.rsqrt(square_sums[0] / model_width + norm_epsilon)[:, None]
    key_scale = lax.rsqrt(square_sums[1] / model_width + norm_epsilon)[:, None]
    query_hat = projected[0] * query_scale
    key_hat = projected[1] * key_scale
    query_gain = qk_gains[0].T.reshape(local_width)
    key_gain = qk_gains[1].T.reshape(local_width)
    positions_all = doc_positions(segments)
    positions = lax.dynamic_slice_in_dim(
        positions_all, context_index * row_count, row_count, axis=1
    ).reshape(token_count)
    cosine, sine_table = rotary_tables(positions)
    cosine = cosine[:, None, :]
    sine_table = sine_table[:, None, :]
    head_shape = (seq_count, row_count, head_count, HEAD_DIM)
    query_rot = (
        rotate(
            (query_hat * query_gain).reshape(token_count, head_count, HEAD_DIM), cosine, sine_table
        )
        .astype(jnp.bfloat16)
        .reshape(head_shape)
    )
    key_rot = (
        rotate((key_hat * key_gain).reshape(token_count, head_count, HEAD_DIM), cosine, sine_table)
        .astype(jnp.bfloat16)
        .reshape(head_shape)
    )
    value_low = projected[2].astype(jnp.bfloat16).reshape(head_shape)
    earlier_keys, earlier_values = passed_along((key_rot, value_low), "context", 1)
    keys_all = jnp.concatenate([earlier_keys, key_rot], axis=1)
    values_all = jnp.concatenate([earlier_values, value_low], axis=1)
    query_places = context_index * row_count + jnp.arange(row_count, dtype=jnp.int32)
    key_places = (context_index - 1) * row_count + jnp.arange(2 * row_count, dtype=jnp.int32)
    query_segments = jnp.take(segments, query_places, axis=1)
    key_segments = jnp.take(segments, jnp.maximum(key_places, 0), axis=1)
    allowed = (
        (query_segments[:, :, None] == key_segments[:, None, :])
        & (key_places[None, None, :] >= 0)
        & (key_places[None, None, :] <= query_places[None, :, None])
    )
    allowed = allowed[:, None]
    score_factor = HEAD_DIM ** (-0.5)

    def masked_scores():
        plain_scores = (
            jnp.einsum("sqhd,skhd->shqk", query_rot, keys_all, preferred_element_type=jnp.float32)
            * score_factor
        )
        return jnp.where(allowed, plain_scores, masked_score)

    scores = masked_scores()
    score_max = jnp.max(scores, axis=-1, keepdims=True)
    raised = jnp.exp(scores - score_max)
    score_total = jnp.sum(raised, axis=-1, keepdims=True)
    log_total = score_max + jnp.log(score_total)
    weights_low = (raised / score_total).astype(jnp.bfloat16)
    attended = jnp.einsum(
        "shqk,skhd->sqhd", weights_low, values_all, preferred_element_type=jnp.float32
    )
    attended_low = attended.astype(jnp.bfloat16).reshape(token_count, local_width)
    attn_part = jnp.dot(attended_low, out_full, preferred_element_type=jnp.float32)
    tokens_slice = my_slice(flat_tokens, 1)
    attn_slice = sum_ranks(attn_part.astype(jnp.bfloat16), rank)
    hidden_slice = tokens_slice + attn_slice
    square_two = total_over(jnp.sum(hidden_slice * hidden_slice, axis=-1), "tensor")
    scale_two = lax.rsqrt(square_two / model_width + norm_epsilon)[:, None]
    hat_two = hidden_slice * scale_two
    gain_two = my_slice(norm_gains[1], 0)
    normed_slice = (hat_two * gain_two).astype(jnp.bfloat16)
    expert_ids = jnp.arange(EXPERTS, dtype=jnp.int32)
    chunk_normed, chunk_units, chunk_grads = [], [], []
    normed_sum = None
    moe_slice = None

    def expert_mix(units):
        return lax.dot_general(
            units, down_full, (((1,), (1,)), ((), ())), preferred_element_type=jnp.float32
        ).astype(jnp.bfloat16)

    probs_total = jnp.zeros((token_count, EXPERTS), jnp.float32)
    sums = None
    for mask in range(shards):
        normed_source, grad_source = normed_slice, grad_slice
        if streamed and mask:
            normed_source, grad_source, sums, normed_sum, moe_slice = lax.optimization_barrier(
                (normed_source, grad_source, sums, normed_sum, moe_slice)
            )
        part = normed_source if mask == 0 else crossed(normed_source, "shard", mask)
        normed_chunk = spread_ranks(part, rank)
        if streamed and mask:
            grad_chunk = spread_ranks(crossed(grad_source, "shard", mask), rank)
        else:
            grad_chunk = grad_chunks[mask]
        logits = jnp.einsum(
            "td,ed->te", normed_chunk, router_full, preferred_element_type=jnp.float32
        )
        probs = softmax_rows(logits)
        member = jnp.any(route_chunks[mask][:, :, None] == expert_ids, axis=1)
        routed = jnp.where(member, probs, 0.0)
        picked = block_at(routed, shard_index, own_experts, 1)
        member_own = block_at(member.astype(jnp.float32), shard_index, own_experts, 1)
        weight = jnp.concatenate(
            [
                jnp.broadcast_to(picked[:, e : e + 1], (token_count, unit_count))
                for e in range(own_experts)
            ],
            axis=1,
        )
        gate_up_out = jnp.dot(normed_chunk, up_full, preferred_element_type=jnp.float32)
        gate_part = gate_up_out[:, :wide]
        up_part = gate_up_out[:, wide:]
        units_grad = jnp.dot(grad_chunk, down_full, preferred_element_type=jnp.float32)
        gate_sigmoid = jax.nn.sigmoid(gate_part)
        gate_silu = gate_part * gate_sigmoid
        hidden_units = gate_silu * up_part
        weighted_units = (weight * hidden_units).astype(jnp.bfloat16)
        product = hidden_units * units_grad
        picks = member_own * jnp.stack(
            [
                jnp.sum(product[:, e * unit_count : (e + 1) * unit_count], axis=1)
                for e in range(own_experts)
            ],
            axis=1,
        )
        units_grad = units_grad * weight
        gate_grad = units_grad * up_part * gate_sigmoid * (1.0 + gate_part * (1.0 - gate_sigmoid))
        up_grad = units_grad * gate_silu
        both_grad = jnp.concatenate([gate_grad, up_grad], axis=1).astype(jnp.bfloat16)
        normed_part = lax.dot_general(
            both_grad, up_full, (((1,), (1,)), ((), ())), preferred_element_type=jnp.float32
        ).astype(jnp.bfloat16)
        back = sum_ranks(normed_part, rank)
        if mask:
            back = crossed(back.astype(jnp.bfloat16), "shard", mask).astype(jnp.float32)
            picks = crossed(picks, "shard", mask)
        normed_sum = back if normed_sum is None else normed_sum + back
        probs_total = put_at(probs_total, picks, (shard_index ^ mask) * own_experts, 1)
        if mask == 0:
            router_probs = probs
        if streamed:
            terms = [
                half_product(left, right, part_index)
                for left, right in ((normed_chunk, both_grad), (grad_chunk, weighted_units))
                for part_index in (1 - context_index, context_index)
            ]
            sums = terms if sums is None else [old + new for old, new in zip(sums, terms)]
            mixed = sum_ranks(expert_mix(weighted_units), rank)
            if mask:
                mixed = crossed(mixed.astype(jnp.bfloat16), "shard", mask).astype(jnp.float32)
            moe_slice = mixed if mask == 0 else moe_slice + mixed
        else:
            chunk_normed.append(normed_chunk)
            chunk_units.append(weighted_units)
            chunk_grads.append(both_grad)
    probs_grad = total_over(probs_total, "tensor")
    if streamed:
        up_sum = joined_halves(sums[0], sums[1])
        down_sum = joined_halves(sums[2], sums[3])
    else:
        normed_all = jnp.concatenate(chunk_normed, axis=0)
        grad_all = jnp.concatenate(grad_chunks, axis=0)
        units_all = jnp.concatenate(chunk_units, axis=0)
        grads_all = jnp.concatenate(chunk_grads, axis=0)
        up_sum = shared_gradient(normed_all, grads_all, shard_index, context_index)
        down_sum = shared_gradient(grad_all, units_all, shard_index, context_index)
    up_share = expert_shares(up_sum, shard_index, own_experts)
    down_share = expert_shares(down_sum, shard_index, own_experts)
    gate_up_grad_out = (
        up_share.reshape(shards, -1, 2, own_experts, unit_count)
        .transpose(0, 3, 1, 2, 4)
        .reshape(EXPERTS, -1, 2, unit_count)
    )
    down_grad_out = (
        down_share.reshape(shards, -1, own_experts, unit_count)
        .transpose(0, 2, 1, 3)
        .reshape(EXPERTS, -1, unit_count)
    )
    if not streamed:
        mixed = sum_ranks(expert_mix(units_all), rank)
        moe_slice = mixed[:token_count]
        mixed = mixed.astype(jnp.bfloat16)
        for mask in range(1, shards):
            came = crossed(mixed[mask * token_count : (mask + 1) * token_count], "shard", mask)
            moe_slice = moe_slice + came.astype(jnp.float32)
    output = spread_ranks((hidden_slice + moe_slice).astype(jnp.bfloat16), rank).reshape(
        seq_count, row_count, model_width
    )
    logits_grad = router_probs * (
        probs_grad - jnp.sum(router_probs * probs_grad, axis=-1, keepdims=True)
    )
    logits_low = logits_grad.astype(jnp.bfloat16)
    normed_grad = normed_sum + jnp.dot(
        logits_low, my_slice(router_full, 1), preferred_element_type=jnp.float32
    )
    router_term = jnp.einsum(
        "te,td->ed", logits_low, normed_slice, preferred_element_type=jnp.float32
    )
    gain_two_term = jnp.sum(normed_grad * hat_two, axis=0)
    hat_grad = normed_grad * gain_two
    hat_mean = total_over(jnp.sum(hat_grad * hat_two, axis=-1), "tensor")[:, None] / model_width
    hidden_grad = grad_slice.astype(jnp.float32) + scale_two * (hat_grad - hat_two * hat_mean)
    attn_grad_low = spread_ranks(hidden_grad.astype(jnp.bfloat16), rank)
    out_share = shard_sum(
        shared_gradient(attn_grad_low, attended_low, shard_index, context_index), 0, shard_index
    ).T
    attended_grad = (
        jnp.einsum("td,fd->tf", attn_grad_low, out_full, preferred_element_type=jnp.float32)
        .astype(jnp.bfloat16)
        .reshape(head_shape)
    )
    weights_full = jnp.exp(masked_scores() - log_total)
    weights_grad = jnp.einsum(
        "sqhd,skhd->shqk", attended_grad, values_all, preferred_element_type=jnp.float32
    )
    score_grad = (
        weights_full * (weights_grad - jnp.sum(weights_full * weights_grad, axis=-1, keepdims=True))
    ).astype(jnp.bfloat16)
    query_grad = (
        jnp.einsum("shqk,skhd->sqhd", score_grad, keys_all, preferred_element_type=jnp.float32)
        * score_factor
    )
    key_grad_all = (
        jnp.einsum("shqk,sqhd->skhd", score_grad, query_rot, preferred_element_type=jnp.float32)
        * score_factor
    )
    value_grad_all = jnp.einsum(
        "shqk,sqhd->skhd",
        weights_full.astype(jnp.bfloat16),
        attended_grad,
        preferred_element_type=jnp.float32,
    )
    later_keys, later_values = passed_along(
        (key_grad_all[:, :row_count], value_grad_all[:, :row_count]), "context", -1
    )
    key_grad = key_grad_all[:, row_count:] + later_keys
    value_grad = value_grad_all[:, row_count:] + later_values
    query_normed_grad = rotate_back(
        query_grad.reshape(token_count, head_count, HEAD_DIM), cosine, sine_table
    ).reshape(token_count, local_width)
    key_normed_grad = rotate_back(
        key_grad.reshape(token_count, head_count, HEAD_DIM), cosine, sine_table
    ).reshape(token_count, local_width)
    query_gain_term = jnp.sum(query_normed_grad * query_hat, axis=0)
    key_gain_term = jnp.sum(key_normed_grad * key_hat, axis=0)
    qk_term = jnp.stack(
        [
            query_gain_term.reshape(head_count, HEAD_DIM).T,
            key_gain_term.reshape(head_count, HEAD_DIM).T,
        ]
    )
    query_hat_grad = query_normed_grad * query_gain
    key_hat_grad = key_normed_grad * key_gain
    cross_sums = total_over(
        jnp.stack(
            [jnp.sum(query_hat_grad * query_hat, axis=-1), jnp.sum(key_hat_grad * key_hat, axis=-1)]
        ),
        "tensor",
    )
    query_raw_grad = query_scale * (
        query_hat_grad - query_hat * (cross_sums[0] / model_width)[:, None]
    )
    key_raw_grad = key_scale * (key_hat_grad - key_hat * (cross_sums[1] / model_width)[:, None])
    projected_grad = jnp.concatenate(
        [query_raw_grad, key_raw_grad, value_grad.reshape(token_count, local_width)], axis=1
    ).astype(jnp.bfloat16)
    qkv_share = shard_sum(
        shared_gradient(inputs, projected_grad, shard_index, context_index), 0, shard_index
    )
    qkv_share = qkv_share.reshape(-1, 3, local_width).transpose(1, 0, 2)
    inputs_part = jnp.einsum(
        "tce,cde->td",
        projected_grad.reshape(token_count, 3, local_width),
        qkv_full,
        preferred_element_type=jnp.float32,
    )
    inputs_grad = sum_ranks(inputs_part.astype(jnp.bfloat16), rank)
    hat_one_slice = my_slice(hat_one, 1)
    gain_one_term = jnp.sum(inputs_grad * hat_one_slice, axis=0)
    hat_one_grad = inputs_grad * my_slice(norm_gains[0], 0)
    mean_one = (
        total_over(jnp.sum(hat_one_grad * hat_one_slice, axis=-1), "tensor")[:, None] / model_width
    )
    input_grad = spread_ranks(
        (hidden_grad + scale_one * (hat_one_grad - hat_one_slice * mean_one)).astype(jnp.bfloat16),
        rank,
    )

    def small_share(part):
        total = tree_total(tree_total(part, "context"), "shard")
        total = spread_ranks(total, rank)
        share = model_width // (2 * shards)
        return block_at(total, shard_index * 2 + context_index, share, 1)

    router_share = small_share(jnp.concatenate([router_term, gain_two_term[None]], axis=0))
    gain_one_share = small_share(gain_one_term[None])
    qk_total = tree_total(tree_total(qk_term, "context"), "shard")
    return (
        output,
        input_grad.reshape(seq_count, row_count, model_width),
        qkv_share,
        out_share,
        router_share[:EXPERTS],
        jnp.concatenate([gain_one_share, router_share[EXPERTS:]], axis=0),
        block_at(qk_total, shard_index * 2 + context_index, HEAD_DIM // (2 * shards), 1),
        gate_up_grad_out,
        down_grad_out,
    )


def solution(mesh):
    return jax.shard_map(
        local,
        mesh=mesh,
        in_specs=(
            P("shard", "context", None),
            P(None, "shard", "tensor"),
            P("tensor", "shard"),
            P(None, "shard"),
            P(),
            P(None, None, "tensor"),
            P(None, "shard", None, "tensor"),
            P(None, "shard", "tensor"),
            P("shard", "context", None),
            P("shard", None),
            P("shard", "context", None),
        ),
        out_specs=(
            P("shard", "context", None),
            P("shard", "context", None),
            P(None, ("shard", "context"), "tensor"),
            P("tensor", ("shard", "context")),
            P(None, ("shard", "context")),
            P(None, ("shard", "context")),
            P(None, ("shard", "context"), "tensor"),
            P(None, ("shard", "context"), None, "tensor"),
            P(None, ("shard", "context"), "tensor"),
        ),
        check_vma=False,
    )
```

```python
import jax
import jax.numpy as jnp
from jax import lax
from jax.sharding import PartitionSpec as P

SHARD, CONTEXT, TENSOR = "shard", "context", "tensor"
HEAD_DIM = 128
EXPERTS = 16
DOCS = 4


norm_epsilon = 1e-05
rope_base = 10000.0
masked_score = -1e30


def rms_scale(values):
    return lax.rsqrt(jnp.mean(values * values, axis=-1, keepdims=True) + norm_epsilon)


def softmax_rows(scores):
    shifted = scores - jnp.max(scores, axis=-1, keepdims=True)
    raised = jnp.exp(shifted)
    return raised / jnp.sum(raised, axis=-1, keepdims=True)


def doc_positions(segment_rows):
    length = segment_rows.shape[-1]
    docs_list = jnp.arange(DOCS, dtype=jnp.int32)
    member = (segment_rows[..., :, None] == docs_list).astype(jnp.int32)
    sizes_of = jnp.sum(member, axis=-2)
    starts = jnp.cumsum(sizes_of, axis=-1) - sizes_of
    start_of = jnp.sum(member * starts[..., None, :], axis=-1)
    return jnp.arange(length, dtype=jnp.int32) - start_of


def rotary_tables(positions):
    half_dim = HEAD_DIM // 2
    ladder = jnp.arange(half_dim, dtype=jnp.float32)
    inverse = rope_base ** (-2.0 * ladder / HEAD_DIM)
    angles = positions.astype(jnp.float32)[..., None] * inverse
    angles = jnp.concatenate([angles, angles], axis=-1)
    return (jnp.cos(angles), jnp.sin(angles))


def rotate(values, cosine, sine_table):
    half_dim = values.shape[-1] // 2
    lower_half = values[..., :half_dim]
    upper_half = values[..., half_dim:]
    return values * cosine + jnp.concatenate([-upper_half, lower_half], axis=-1) * sine_table


def rotate_back(grad_values, cosine, sine_table):
    half_dim = grad_values.shape[-1] // 2
    turned = grad_values * sine_table
    return grad_values * cosine + jnp.concatenate(
        [turned[..., half_dim:], -turned[..., :half_dim]], axis=-1
    )


def passed_along(value, axis, by):
    length = lax.axis_size(axis)
    pairs = [(i, i + by) for i in range(length) if 0 <= i + by < length]
    return lax.ppermute(value, axis, pairs)


def crossed(value, axis, mask):
    length = lax.axis_size(axis)
    return lax.ppermute(value, axis, [(i, i ^ mask) for i in range(length)])


def block_at(value, index, size, axis):
    return lax.dynamic_slice_in_dim(value, index * size, size, axis=axis)


def put_at(whole, part, start, axis):
    return lax.dynamic_update_slice_in_dim(whole, part, start, axis=axis)


def after(value, *gates):
    return lax.optimization_barrier((value, gates))[0]


def after_each(values, *gates):
    return [after(value, *gates) for value in values]


def fetch(targets, axis, shard_index, context_index):
    size = targets(0).shape[axis] // 2
    pieces = []
    for mask in range(1, lax.axis_size(SHARD)):
        block = block_at(targets(shard_index ^ mask), context_index, size, axis)
        pieces.append(crossed(block, SHARD, mask))
    return pieces


def assemble(own, pieces, axis, shard_index, context_index):
    size = own.shape[axis]
    half = size // 2
    shape = list(own.shape)
    shape[axis] = size * lax.axis_size(SHARD)
    whole = put_at(jnp.zeros(shape, own.dtype), own, shard_index * size, axis)
    for mask, came in enumerate(pieces, 1):
        partner = shard_index ^ mask
        other = crossed(came, CONTEXT, 1)
        whole = put_at(whole, came, partner * size + context_index * half, axis)
        whole = put_at(whole, other, partner * size + (1 - context_index) * half, axis)
    return whole


def spread_ranks(part, rank):
    rows, width = part.shape
    ranks = lax.axis_size(TENSOR)
    whole = jnp.zeros((rows, ranks * width), part.dtype)
    whole = put_at(whole, part, rank * width, 1)
    for mask in range(1, ranks):
        whole = put_at(whole, crossed(part, TENSOR, mask), (rank ^ mask) * width, 1)
    return whole


def sum_ranks(value, rank):
    ranks = lax.axis_size(TENSOR)
    width = value.shape[1] // ranks
    total = block_at(value, rank, width, 1).astype(jnp.float32)
    for mask in range(1, ranks):
        came = crossed(block_at(value, rank ^ mask, width, 1), TENSOR, mask)
        total = total + came.astype(jnp.float32)
    return total


def total_over(value, axis):
    total = value
    for mask in range(1, lax.axis_size(axis)):
        total = total + crossed(value, axis, mask)
    return total


def column_half(value, part, shards):
    size = value.shape[1] // (2 * shards)
    return jnp.concatenate(
        [lax.dynamic_slice_in_dim(value, (2 * p + part) * size, size, axis=1) for p in range(shards)],
        axis=1,
    )


def half_product(left, right, part):
    return lax.dot_general(
        column_half(left, part, lax.axis_size(SHARD)),
        right,
        (((0,), (0,)), ((), ())),
        preferred_element_type=jnp.float32,
    )


def joined_halves(give, keep):
    came = crossed(give.astype(jnp.bfloat16), CONTEXT, 1)
    total = keep + came.astype(jnp.float32)
    return total, total.astype(jnp.bfloat16)


def shared_gradient(left, right, context_index):
    give = half_product(left, right, 1 - context_index).astype(jnp.bfloat16)
    keep = half_product(left, right, context_index)
    return (give,) + joined_halves(give, keep)


def shard_sum(value, low, axis, shard_index):
    shards = lax.axis_size(SHARD)
    size = value.shape[axis] // shards
    total = block_at(value, shard_index, size, axis)
    for mask in range(1, shards):
        came = crossed(block_at(low, shard_index ^ mask, size, axis), SHARD, mask)
        total = total + came.astype(jnp.float32)
    return total


def expert_shares(value, low, shard_index, split):
    shards = lax.axis_size(SHARD)
    rows = value.shape[0] // shards
    own = split(block_at(value, shard_index, rows, 0))
    count = own.shape[0]
    result = jnp.zeros((EXPERTS,) + own.shape[1:], jnp.float32)
    result = put_at(result, own, shard_index * count, 0)
    for mask in range(1, shards):
        partner = shard_index ^ mask
        came = crossed(block_at(low, partner, rows, 0), SHARD, mask)
        result = put_at(result, split(came.astype(jnp.float32)), partner * count, 0)
    return result


def local(
    tokens,
    qkv_weight,
    out_weight,
    router_weight,
    norm_gains,
    qk_gains,
    gate_up_weight,
    down_weight,
    routes,
    segments,
    cotangent,
):
    seq_count, row_count, model_width = tokens.shape
    token_count = seq_count * row_count
    top_count = routes.shape[2]
    local_width = qkv_weight.shape[2]
    head_count = local_width // HEAD_DIM
    shards = lax.axis_size(SHARD)
    ranks = lax.axis_size(TENSOR)
    own_experts = EXPERTS // shards
    unit_count = down_weight.shape[2]
    wide = own_experts * unit_count
    slice_width = model_width // ranks
    context_index = lax.axis_index(CONTEXT)
    shard_index = lax.axis_index(SHARD)
    rank = lax.axis_index(TENSOR)

    def my_slice(value, axis):
        return block_at(value, rank, slice_width, axis)

    qkv_pieces = fetch(lambda target: qkv_weight, 1, shard_index, context_index)
    qkv_full = assemble(qkv_weight, qkv_pieces, 1, shard_index, context_index)
    out_gated = after(out_weight, *qkv_pieces)
    out_pieces = fetch(lambda target: out_gated, 1, shard_index, context_index)
    router_size = router_weight.shape[1]
    router_full = jnp.zeros((EXPERTS, model_width), router_weight.dtype)
    router_full = put_at(router_full, router_weight, shard_index * router_size, 1)
    for mask in range(1, shards):
        came = crossed(router_weight, SHARD, mask)
        router_full = put_at(router_full, came, (shard_index ^ mask) * router_size, 1)
    route_rows = routes.reshape(token_count, top_count)
    grad_low = cotangent.reshape(token_count, model_width)
    grad_slice = my_slice(grad_low, 1)
    up_lines = gate_up_weight.transpose(1, 2, 0, 3).reshape(-1, 2, shards, wide)
    down_lines = down_weight.transpose(1, 0, 2).reshape(-1, shards, wide)
    streamed = shards * token_count * model_width > 8 * 1024 * 1024
    grad_chunks = [grad_low]
    route_chunks = [route_rows] + [crossed(route_rows, SHARD, mask) for mask in range(1, shards)]
    flat_tokens = tokens.reshape(token_count, model_width).astype(jnp.float32)
    scale_one = rms_scale(flat_tokens)
    hat_one = flat_tokens * scale_one
    inputs = (hat_one * norm_gains[0]).astype(jnp.bfloat16)
    projected = jnp.einsum(
        "td,cde->cte", inputs, qkv_full, preferred_element_type=jnp.float32
    )

    up_gated, down_gated = after((up_lines, down_lines), *qkv_pieces)

    def up_block(target, lines=up_gated):
        return lax.dynamic_index_in_dim(lines, target, 2, False).reshape(-1, 2 * wide)

    def down_block(target, lines=down_gated):
        return lax.dynamic_index_in_dim(lines, target, 1, False)

    up_pieces = fetch(up_block, 0, shard_index, context_index)
    down_pieces = fetch(down_block, 0, shard_index, context_index)
    out_pieces = after_each(out_pieces, projected)
    out_full = assemble(out_weight, out_pieces, 1, shard_index, context_index)

    square_sums = total_over(jnp.sum(projected[:2] * projected[:2], axis=-1), TENSOR)
    query_scale = lax.rsqrt(square_sums[0] / model_width + norm_epsilon)[:, None]
    key_scale = lax.rsqrt(square_sums[1] / model_width + norm_epsilon)[:, None]
    query_hat = projected[0] * query_scale
    key_hat = projected[1] * key_scale
    query_gain = qk_gains[0].T.reshape(local_width)
    key_gain = qk_gains[1].T.reshape(local_width)
    positions_all = doc_positions(segments)
    positions = lax.dynamic_slice_in_dim(
        positions_all, context_index * row_count, row_count, axis=1
    ).reshape(token_count)
    cosine, sine_table = rotary_tables(positions)
    cosine = cosine[:, None, :]
    sine_table = sine_table[:, None, :]
    head_shape = (seq_count, row_count, head_count, HEAD_DIM)
    query_rot = (
        rotate(
            (query_hat * query_gain).reshape(token_count, head_count, HEAD_DIM), cosine, sine_table
        )
        .astype(jnp.bfloat16)
        .reshape(head_shape)
    )
    key_rot = (
        rotate((key_hat * key_gain).reshape(token_count, head_count, HEAD_DIM), cosine, sine_table)
        .astype(jnp.bfloat16)
        .reshape(head_shape)
    )
    value_low = projected[2].astype(jnp.bfloat16).reshape(head_shape)
    earlier_keys, earlier_values = passed_along((key_rot, value_low), CONTEXT, 1)
    keys_all = jnp.concatenate([earlier_keys, key_rot], axis=1)
    values_all = jnp.concatenate([earlier_values, value_low], axis=1)
    query_places = context_index * row_count + jnp.arange(row_count, dtype=jnp.int32)
    key_places = (context_index - 1) * row_count + jnp.arange(2 * row_count, dtype=jnp.int32)
    query_segments = jnp.take(segments, query_places, axis=1)
    key_segments = jnp.take(segments, jnp.maximum(key_places, 0), axis=1)
    allowed = (
        (query_segments[:, :, None] == key_segments[:, None, :])
        & (key_places[None, None, :] >= 0)
        & (key_places[None, None, :] <= query_places[None, :, None])
    )
    allowed = allowed[:, None]
    score_factor = HEAD_DIM ** (-0.5)

    def masked_scores():
        plain_scores = (
            jnp.einsum("sqhd,skhd->shqk", query_rot, keys_all, preferred_element_type=jnp.float32)
            * score_factor
        )
        return jnp.where(allowed, plain_scores, masked_score)

    scores = masked_scores()
    score_max = jnp.max(scores, axis=-1, keepdims=True)
    raised = jnp.exp(scores - score_max)
    score_total = jnp.sum(raised, axis=-1, keepdims=True)
    log_total = score_max + jnp.log(score_total)
    weights_low = (raised / score_total).astype(jnp.bfloat16)
    attended = jnp.einsum(
        "shqk,skhd->sqhd", weights_low, values_all, preferred_element_type=jnp.float32
    )
    attended_low = attended.astype(jnp.bfloat16).reshape(token_count, local_width)
    attn_part = jnp.dot(attended_low, out_full, preferred_element_type=jnp.float32)
    tokens_slice = my_slice(flat_tokens, 1)
    attn_slice = sum_ranks(attn_part.astype(jnp.bfloat16), rank)
    hidden_slice = tokens_slice + attn_slice
    square_two = total_over(jnp.sum(hidden_slice * hidden_slice, axis=-1), TENSOR)
    scale_two = lax.rsqrt(square_two / model_width + norm_epsilon)[:, None]
    hat_two = hidden_slice * scale_two
    gain_two = my_slice(norm_gains[1], 0)
    normed_slice = (hat_two * gain_two).astype(jnp.bfloat16)
    up_pieces = after_each(up_pieces, normed_slice)
    down_pieces = after_each(down_pieces, normed_slice)
    up_full = assemble(up_block(shard_index, up_lines), up_pieces, 0, shard_index, context_index)
    down_full = assemble(
        down_block(shard_index, down_lines), down_pieces, 0, shard_index, context_index
    )
    normed_pieces, grad_pieces = [], []
    if not streamed:
        normed_gated = after(normed_slice, up_pieces[-1])
        normed_pieces = [crossed(normed_gated, SHARD, mask) for mask in range(1, shards)]
        grad_gated = after(grad_slice, normed_pieces[:1])
        grad_pieces = [crossed(grad_gated, SHARD, mask) for mask in range(1, shards)]
    expert_ids = jnp.arange(EXPERTS, dtype=jnp.int32)
    chunk_normed, chunk_units, chunk_grads = [], [], []
    parts_made = []
    normed_sum = None
    moe_slice = None

    def expert_mix(units):
        return lax.dot_general(
            units, down_full, (((1,), (1,)), ((), ())), preferred_element_type=jnp.float32
        ).astype(jnp.bfloat16)

    probs_total = jnp.zeros((token_count, EXPERTS), jnp.float32)
    sums = None
    for mask in range(shards):
        normed_source, grad_source = normed_slice, grad_slice
        if streamed and mask:
            normed_source, grad_source, sums, normed_sum, moe_slice = lax.optimization_barrier(
                (normed_source, grad_source, sums, normed_sum, moe_slice)
            )
        if streamed:
            part = normed_source if mask == 0 else crossed(normed_source, SHARD, mask)
            normed_chunk = spread_ranks(part, rank)
        elif mask == 0:
            normed_chunk = spread_ranks(normed_slice, rank)
        else:
            normed_chunk = normed_chunks[mask]
        if streamed and mask:
            grad_chunk = spread_ranks(crossed(grad_source, SHARD, mask), rank)
        else:
            grad_chunk = grad_chunks[mask]
        logits = jnp.einsum(
            "td,ed->te", normed_chunk, router_full, preferred_element_type=jnp.float32
        )
        probs = softmax_rows(logits)
        member = jnp.any(route_chunks[mask][:, :, None] == expert_ids, axis=1)
        routed = jnp.where(member, probs, 0.0)
        picked = block_at(routed, shard_index, own_experts, 1)
        member_own = block_at(member.astype(jnp.float32), shard_index, own_experts, 1)
        weight = jnp.concatenate(
            [
                jnp.broadcast_to(picked[:, e : e + 1], (token_count, unit_count))
                for e in range(own_experts)
            ],
            axis=1,
        )
        gate_up_out = jnp.dot(normed_chunk, up_full, preferred_element_type=jnp.float32)
        gate_part = gate_up_out[:, :wide]
        up_part = gate_up_out[:, wide:]
        units_grad = jnp.dot(grad_chunk, down_full, preferred_element_type=jnp.float32)
        gate_sigmoid = jax.nn.sigmoid(gate_part)
        gate_silu = gate_part * gate_sigmoid
        hidden_units = gate_silu * up_part
        weighted_units = (weight * hidden_units).astype(jnp.bfloat16)
        product = hidden_units * units_grad
        picks = member_own * jnp.stack(
            [
                jnp.sum(product[:, e * unit_count : (e + 1) * unit_count], axis=1)
                for e in range(own_experts)
            ],
            axis=1,
        )
        units_grad = units_grad * weight
        gate_grad = units_grad * up_part * gate_sigmoid * (1.0 + gate_part * (1.0 - gate_sigmoid))
        up_grad = units_grad * gate_silu
        both_grad = jnp.concatenate([gate_grad, up_grad], axis=1).astype(jnp.bfloat16)
        normed_part = lax.dot_general(
            both_grad, up_full, (((1,), (1,)), ((), ())), preferred_element_type=jnp.float32
        ).astype(jnp.bfloat16)
        parts_made.append(normed_part)
        if mask == 0 and not streamed:
            normed_pieces = after_each(normed_pieces, normed_part)
            normed_chunks = [normed_chunk] + [spread_ranks(piece, rank) for piece in normed_pieces]
            grad_pieces = [after(one, other) for one, other in zip(grad_pieces, normed_pieces)]
            grad_chunks = grad_chunks + [spread_ranks(piece, rank) for piece in grad_pieces]
        if mask:
            back = sum_ranks(normed_part, rank)
            back = crossed(back.astype(jnp.bfloat16), SHARD, mask).astype(jnp.float32)
            picks = crossed(picks, SHARD, mask)
            normed_sum = back if normed_sum is None else normed_sum + back
        elif streamed:
            normed_sum = sum_ranks(normed_part, rank)
        probs_total = put_at(probs_total, picks, (shard_index ^ mask) * own_experts, 1)
        if mask == 0:
            router_probs = probs
        if streamed:
            terms = [
                half_product(left, right, part_index)
                for left, right in ((normed_chunk, both_grad), (grad_chunk, weighted_units))
                for part_index in (1 - context_index, context_index)
            ]
            sums = terms if sums is None else [old + new for old, new in zip(sums, terms)]
            mixed = sum_ranks(expert_mix(weighted_units), rank)
            if mask:
                mixed = crossed(mixed.astype(jnp.bfloat16), SHARD, mask).astype(jnp.float32)
            moe_slice = mixed if mask == 0 else moe_slice + mixed
        else:
            chunk_normed.append(normed_chunk)
            chunk_units.append(weighted_units)
            chunk_grads.append(both_grad)
    if not streamed:
        own_back = sum_ranks(after(parts_made[0], parts_made[1:]), rank)
        normed_sum = own_back if normed_sum is None else own_back + normed_sum
    probs_grad = total_over(probs_total, TENSOR)
    if streamed:
        up_sum, up_low = joined_halves(sums[0], sums[1])
        down_sum, down_low = joined_halves(sums[2], sums[3])
    else:
        chunk_units, chunk_grads = after((chunk_units, chunk_grads), parts_made)
        normed_all = jnp.concatenate(chunk_normed, axis=0)
        grad_all = jnp.concatenate(grad_chunks, axis=0)
        units_all = jnp.concatenate(chunk_units, axis=0)
        grads_all = jnp.concatenate(chunk_grads, axis=0)
        mixed = expert_mix(units_all)
        mixed_made = mixed
        mixed = sum_ranks(mixed, rank)
        _, up_sum, up_low = shared_gradient(normed_all, grads_all, context_index)
        _, down_sum, down_low = shared_gradient(grad_all, units_all, context_index)
        probs_grad = after(probs_grad, normed_sum, up_low, down_low, mixed_made)
        up_low, down_low = after_each([up_low, down_low], normed_sum)
    gate_up_grad_out = expert_shares(
        up_sum,
        up_low,
        shard_index,
        lambda block: block.reshape(-1, 2, own_experts, unit_count).transpose(2, 0, 1, 3),
    )
    down_grad_out = expert_shares(
        down_sum,
        down_low,
        shard_index,
        lambda block: block.reshape(-1, own_experts, unit_count).transpose(1, 0, 2),
    )
    logits_grad = router_probs * (
        probs_grad - jnp.sum(router_probs * probs_grad, axis=-1, keepdims=True)
    )
    logits_low = logits_grad.astype(jnp.bfloat16)
    normed_grad = normed_sum + jnp.dot(
        logits_low, my_slice(router_full, 1), preferred_element_type=jnp.float32
    )
    router_term = jnp.einsum(
        "te,td->ed", logits_low, normed_slice, preferred_element_type=jnp.float32
    )
    gain_two_term = jnp.sum(normed_grad * hat_two, axis=0)
    hat_grad = normed_grad * gain_two
    hat_mean = total_over(jnp.sum(hat_grad * hat_two, axis=-1), TENSOR)[:, None] / model_width
    hidden_grad = grad_slice.astype(jnp.float32) + scale_two * (hat_grad - hat_two * hat_mean)
    attn_grad_low = spread_ranks(hidden_grad.astype(jnp.bfloat16), rank)
    mixed_pieces = []
    if not streamed:
        moe_slice = mixed[:token_count]
        mixed = mixed.astype(jnp.bfloat16)
        mixed_pieces = [
            crossed(mixed[mask * token_count : (mask + 1) * token_count], SHARD, mask)
            for mask in range(1, shards)
        ]
    out_sum, out_low = shared_gradient(attn_grad_low, attended_low, context_index)[1:]
    out_share = shard_sum(out_sum, out_low, 0, shard_index).T
    attended_grad = jnp.einsum(
        "td,fd->tf", attn_grad_low, out_full, preferred_element_type=jnp.float32
    ).astype(jnp.bfloat16)
    attended_grad = attended_grad.reshape(head_shape)
    weights_full = jnp.exp(masked_scores() - log_total)
    weights_grad = jnp.einsum(
        "sqhd,skhd->shqk", attended_grad, values_all, preferred_element_type=jnp.float32
    )
    score_grad = (
        weights_full * (weights_grad - jnp.sum(weights_full * weights_grad, axis=-1, keepdims=True))
    ).astype(jnp.bfloat16)
    query_grad = (
        jnp.einsum("shqk,skhd->sqhd", score_grad, keys_all, preferred_element_type=jnp.float32)
        * score_factor
    )
    key_grad_all = (
        jnp.einsum("shqk,sqhd->skhd", score_grad, query_rot, preferred_element_type=jnp.float32)
        * score_factor
    )
    value_grad_all = jnp.einsum(
        "shqk,sqhd->skhd",
        weights_full.astype(jnp.bfloat16),
        attended_grad,
        preferred_element_type=jnp.float32,
    )
    later_keys, later_values = passed_along(
        (key_grad_all[:, :row_count], value_grad_all[:, :row_count]), CONTEXT, -1
    )
    key_grad = key_grad_all[:, row_count:] + later_keys
    value_grad = value_grad_all[:, row_count:] + later_values
    query_normed_grad = rotate_back(
        query_grad.reshape(token_count, head_count, HEAD_DIM), cosine, sine_table
    ).reshape(token_count, local_width)
    key_normed_grad = rotate_back(
        key_grad.reshape(token_count, head_count, HEAD_DIM), cosine, sine_table
    ).reshape(token_count, local_width)
    query_gain_term = jnp.sum(query_normed_grad * query_hat, axis=0)
    key_gain_term = jnp.sum(key_normed_grad * key_hat, axis=0)
    qk_term = jnp.stack(
        [
            query_gain_term.reshape(head_count, HEAD_DIM).T,
            key_gain_term.reshape(head_count, HEAD_DIM).T,
        ]
    )
    query_hat_grad = query_normed_grad * query_gain
    key_hat_grad = key_normed_grad * key_gain
    cross_sums = total_over(
        jnp.stack(
            [jnp.sum(query_hat_grad * query_hat, axis=-1), jnp.sum(key_hat_grad * key_hat, axis=-1)]
        ),
        TENSOR,
    )
    query_raw_grad = query_scale * (
        query_hat_grad - query_hat * (cross_sums[0] / model_width)[:, None]
    )
    key_raw_grad = key_scale * (key_hat_grad - key_hat * (cross_sums[1] / model_width)[:, None])
    projected_grad = jnp.concatenate(
        [query_raw_grad, key_raw_grad, value_grad.reshape(token_count, local_width)], axis=1
    ).astype(jnp.bfloat16)
    qkv_sum, qkv_low = shared_gradient(inputs, projected_grad, context_index)[1:]
    qkv_share = shard_sum(qkv_sum, qkv_low, 0, shard_index)
    qkv_share = qkv_share.reshape(-1, 3, local_width).transpose(1, 0, 2)
    inputs_part = jnp.einsum(
        "tce,cde->td",
        projected_grad.reshape(token_count, 3, local_width),
        qkv_full,
        preferred_element_type=jnp.float32,
    )
    inputs_grad = sum_ranks(after(inputs_part.astype(jnp.bfloat16), qkv_low), rank)
    hat_one_slice = my_slice(hat_one, 1)
    gain_one_term = jnp.sum(inputs_grad * hat_one_slice, axis=0)
    hat_one_grad = inputs_grad * my_slice(norm_gains[0], 0)
    mean_one = (
        total_over(jnp.sum(hat_one_grad * hat_one_slice, axis=-1), TENSOR)[:, None] / model_width
    )
    input_low = (hidden_grad + scale_one * (hat_one_grad - hat_one_slice * mean_one)).astype(
        jnp.bfloat16
    )
    input_grad = spread_ranks(input_low, rank)
    for came in after_each(
        mixed_pieces, input_low, gate_up_grad_out[:1, :1, :1, :1], down_grad_out[:1, :1, :1]
    ):
        moe_slice = moe_slice + came.astype(jnp.float32)
    output = spread_ranks((hidden_slice + moe_slice).astype(jnp.bfloat16), rank).reshape(
        seq_count, row_count, model_width
    )
    packed = jnp.concatenate(
        [
            router_term,
            gain_one_term[None],
            gain_two_term[None],
            qk_term.reshape(-1, slice_width),
        ],
        axis=0,
    )
    packed = total_over(total_over(packed, CONTEXT), SHARD)
    own_place = shard_index * 2 + context_index
    small = block_at(
        spread_ranks(packed[: EXPERTS + 2], rank), own_place, model_width // (2 * shards), 1
    )
    qk_total = packed[EXPERTS + 2 :].reshape(qk_term.shape)
    return (
        output,
        input_grad.reshape(seq_count, row_count, model_width),
        qkv_share,
        out_share,
        small[:EXPERTS],
        small[EXPERTS:],
        block_at(qk_total, own_place, HEAD_DIM // (2 * shards), 1),
        gate_up_grad_out,
        down_grad_out,
    )


def solution(mesh):
    return jax.shard_map(
        local,
        mesh=mesh,
        in_specs=(
            P(SHARD, CONTEXT, None),
            P(None, SHARD, TENSOR),
            P(TENSOR, SHARD),
            P(None, SHARD),
            P(),
            P(None, None, TENSOR),
            P(None, SHARD, None, TENSOR),
            P(None, SHARD, TENSOR),
            P(SHARD, CONTEXT, None),
            P(SHARD, None),
            P(SHARD, CONTEXT, None),
        ),
        out_specs=(
            P(SHARD, CONTEXT, None),
            P(SHARD, CONTEXT, None),
            P(None, (SHARD, CONTEXT), TENSOR),
            P(TENSOR, (SHARD, CONTEXT)),
            P(None, (SHARD, CONTEXT)),
            P(None, (SHARD, CONTEXT)),
            P(None, (SHARD, CONTEXT), TENSOR),
            P(None, (SHARD, CONTEXT), None, TENSOR),
            P(None, (SHARD, CONTEXT), TENSOR),
        ),
        check_vma=False,
    )
```
